32 devices in a mesh: sec: 2 (over x), tile: 16 (over z, y, core).
Axes of the slice: x: 2, y: 2, z: 4, core: 2. Of those that a mesh axis runs over, the one named last changes fastest.
Arguments:
- atmosphere: bfloat16 [32, 360, 384], P(('sec', 'tile')), may hold values from -6 to 6
- ocean_state: bfloat16 [128, 1440, 128], P('tile', 'sec'), may hold values from -6 to 6
- land_mask: int32 [128, 1440], P('tile', 'sec'), may hold values 0 or 1
- crossing_bands: int32 [16, 4], P('tile'), may hold values from 0 to 31, as said below
- ocean_regrid: float32 [16, 4, 8, 1], P('tile'), may hold values from 0 to 1, as said below
- atmosphere_regrid: float32 [16, 4, 1, 8], P('tile'), may hold values from 0 to 1, as said below
- surface_read: bfloat16 [128], replicated, may hold values from -0.5 to 0.5
- surface_embed: float32 [384], replicated, may hold values from -4 to 4
- flux_read: bfloat16 [384, 8], replicated, may hold values from -0.3125 to 0.3125
- flux_embed: bfloat16 [8, 128], replicated, may hold values from -2 to 2
- legendre_forward: bfloat16 [128, 32, 32], P(('sec', 'tile')), may hold values from -1 to 1
- legendre_inverse: bfloat16 [128, 32, 32], P(('sec', 'tile')), may hold values from -1 to 1
- spectral_mix: bfloat16 [2, 384, 384], replicated, may hold values from -0.3125 to 0.3125
- conv_kernel: bfloat16 [2, 7, 7, 128], replicated, may hold values from -0.875 to 0.875
- norm_gain: float32 [2, 128], replicated, may hold values from 0.1 to 1.9
- expand_weight: bfloat16 [2, 128, 512], replicated, may hold values from -0.5 to 0.5
- project_weight: bfloat16 [2, 512, 128], replicated, may hold values from -0.25 to 0.25
- atmosphere_cotangent: bfloat16 [32, 360, 384], P(('sec', 'tile')), may hold values from -6 to 6
- ocean_cotangent: bfloat16 [128, 1440, 128], P('tile', 'sec'), may hold values from -6 to 6
Outputs:
- atmosphere_next: bfloat16 [32, 360, 384], P(('sec', 'tile'))
- ocean_next: bfloat16 [128, 1440, 128], P('tile', 'sec')
- atmosphere_grad: float32 [32, 360, 384], P(('sec', 'tile'))
- ocean_grad: float32 [128, 1440, 128], P('tile', 'sec')
The draws below stay inside these ranges and needn't reach their ends.
Inputs may be any that keep to these rules, and one draw needn't show every extreme that they name: `crossing_bands`: row j lists between 1 and 4 consecutive distinct atmosphere bands, then repeats its last band; some row lists 4. Its first band is j * 2 - 1, j * 2 or j * 2 + 1, raised to 0 or lowered as far as needed for the list to end at band 32 - 1 at most. `ocean_regrid`: zero in the repeated slots of crossing_bands; the entries of each ocean row sum to one. `atmosphere_regrid`: zero in the repeated slots of crossing_bands.
All inputs are finite; a program needn't handle non-finite values. No bound on the sum of `land_mask` on one device may be relied on, other than what follows from the above.
Results may differ from the reference program's by a relative error of at most 0.008.
Values may be sent and summed in bfloat16 or wider, within the bound.
A program may use at most 128 MiB of HBM per device.

```python
import jax
import jax.numpy as jnp
from jax import lax

C = 384
ALON = 360
MODES = 128
F = 8
OC = 128
OHID = 512
KS = 7
LAYERS = 2
PEERS = 4
ALAT_DEV = 1
OLAT_DEV = 8
BANDS = 32
GROUPS = 16
ALAT = 32
OLAT = 128
OLON = 1440


def crossing_layout(key):
    base = jax.random.fold_in(key, 17)
    count_key, step_key = jax.random.split(base)
    group_index = jnp.arange(GROUPS, dtype=jnp.int32)
    counts = jax.random.randint(count_key, (GROUPS,), 1, PEERS + 1).astype(jnp.int32)
    counts = jnp.where(group_index == GROUPS // 2, PEERS, counts)
    wiggle = jax.random.randint(step_key, (GROUPS,), -1, 2).astype(jnp.int32)
    first = group_index * (BANDS // GROUPS) + wiggle
    first = jnp.minimum(jnp.maximum(first, 0), BANDS - counts)
    slot = jnp.arange(PEERS, dtype=jnp.int32)
    listed = first[:, None] + jnp.minimum(slot[None, :], counts[:, None] - 1)
    valid = (slot[None, :] < counts[:, None]).astype(jnp.float32)
    return (listed.astype(jnp.int32), valid)


def positive_weights(key, shape):
    raw = jax.random.uniform(key, shape, jnp.float32, 0.2, 1.0)
    return raw


def draw_crossing_bands(key, part):
    return crossing_layout(key)[0]


def draw_ocean_regrid(key, part):
    listed, valid = crossing_layout(key)
    raw = positive_weights(jax.random.fold_in(key, 29), (GROUPS, PEERS, OLAT_DEV, ALAT_DEV))
    raw = raw * valid[:, :, None, None]
    return raw / jnp.sum(raw, axis=(1, 3), keepdims=True)


def draw_atmosphere_regrid(key, part):
    listed, valid = crossing_layout(key)
    raw = positive_weights(jax.random.fold_in(key, 31), (GROUPS, PEERS, ALAT_DEV, OLAT_DEV))
    return raw * valid[:, :, None, None] / OLAT_DEV


def touch_ends(array, own_key, smallest, largest):
    place = [jax.random.randint(jax.random.fold_in(own_key, axis), (), 0, length) for axis, length in enumerate(array.shape)]
    widest = array.shape.index(max(array.shape))
    beside = place[:widest] + [(place[widest] + 1) % array.shape[widest]] + place[widest + 1:]
    return array.at[tuple(place)].set(smallest).at[tuple(beside)].set(largest)


def shard_levels(rng, shape, cuts, least, high):
    def one(axis_at, shards_of):
        steps = jax.random.uniform(jax.random.fold_in(jax.random.fold_in(rng, 6), axis_at), (shards_of,), jnp.float32, least / len(cuts), high / len(cuts))
        return jnp.repeat(jnp.exp(steps), shape[axis_at] // shards_of).reshape((-1,) + (1,) * (len(shape) - axis_at - 1))

    loudness = one(*cuts[0])
    for cut in cuts[1:]:
        loudness = loudness * one(*cut)
    return loudness


def centred(stream_key, shape, deviation, limit, cuts=(), kind=jnp.bfloat16):
    entries = jax.random.normal(stream_key, shape, jnp.float32) * deviation
    if len(cuts) > 0:
        entries = shard_levels(stream_key, shape, cuts, -0.22, 0.18) * entries
    return jnp.clip(entries, min=-limit, max=limit).astype(kind)


def setup_inputs(seed: int = 0) -> dict:
    arg_keys = jax.random.split(jax.random.key(seed), 20)
    return {
        "atmosphere": centred(arg_keys[0], (ALAT, ALON, C), 1.0, 6.0, ((0, 32),)),
        "ocean_state": centred(arg_keys[1], (OLAT, OLON, OC), 1.0, 6.0, ((0, 16), (1, 2))),
        "land_mask": touch_ends((jax.random.randint(arg_keys[2], (OLAT, OLON), 0, 10) < 7).astype(jnp.int32), jax.random.fold_in(arg_keys[2], 1), 0, 1),
        "crossing_bands": draw_crossing_bands(jax.random.fold_in(arg_keys[19], 71), 0),
        "ocean_regrid": draw_ocean_regrid(jax.random.fold_in(arg_keys[19], 71), 0),
        "atmosphere_regrid": draw_atmosphere_regrid(jax.random.fold_in(arg_keys[19], 71), 0),
        "surface_read": centred(arg_keys[6], (OC,), OC ** -0.5, 0.5),
        "surface_embed": centred(arg_keys[7], (C,), 1.0, 4.0, (), jnp.float32),
        "flux_read": centred(arg_keys[8], (C, F), C ** -0.5, 0.3125),
        "flux_embed": centred(arg_keys[9], (F, OC), F ** -0.5, 2.0),
        "legendre_forward": centred(arg_keys[10], (MODES, ALAT, ALAT), ALAT ** -0.5, 1.0, ((0, 32),)),
        "legendre_inverse": centred(arg_keys[11], (MODES, ALAT, ALAT), ALAT ** -0.5, 1.0, ((0, 32),)),
        "spectral_mix": centred(arg_keys[12], (2, C, C), C ** -0.5, 0.3125),
        "conv_kernel": centred(arg_keys[13], (LAYERS, KS, KS, OC), (KS * KS) ** -0.5, 0.875),
        "norm_gain": jnp.clip(1.0 + 0.18 * jax.random.normal(arg_keys[14], (LAYERS, OC), jnp.float32), 0.1, 1.9),
        "expand_weight": centred(arg_keys[15], (LAYERS, OC, OHID), OC ** -0.5, 0.5),
        "project_weight": centred(arg_keys[16], (LAYERS, OHID, OC), OHID ** -0.5, 0.25),
        "atmosphere_cotangent": centred(arg_keys[17], (ALAT, ALON, C), 1.0, 6.0, ((0, 32),)),
        "ocean_cotangent": centred(arg_keys[18], (OLAT, OLON, OC), 1.0, 6.0, ((0, 16), (1, 2))),
    }


def wave_table(lon_count, mode_count):
    longitude = jnp.arange(lon_count, dtype=jnp.int32)
    wavenumber = jnp.arange(mode_count, dtype=jnp.int32)
    phase = (longitude[:, None] * wavenumber[None, :] % lon_count).astype(jnp.float32) * (2.0 * jnp.pi / lon_count)
    scaled = jnp.stack([jnp.cos(phase), -jnp.sin(phase)], axis=2) * jnp.sqrt(jnp.float32(2.0 / lon_count))
    return scaled.reshape(lon_count, 2 * mode_count).astype(jnp.bfloat16)

def depthwise(window, kernel):
    radius = kernel.shape[0] // 2
    height = window.shape[0] - 2 * radius
    extent = window.shape[1]
    wide = jnp.concatenate([window[:, extent - radius:], window, window[:, :radius]], axis=1).astype(jnp.float32)
    weights = kernel.astype(jnp.float32)
    total = jnp.zeros((height, extent, window.shape[2]), jnp.float32)
    for shift_row in range(kernel.shape[0]):
        for shift_col in range(kernel.shape[1]):
            total = total + wide[shift_row:shift_row + height, shift_col:shift_col + extent] * weights[shift_row, shift_col]
    return total

def cell_forward(hidden, gain, expand, project):
    center = hidden - lax.optimization_barrier(jnp.mean(hidden, axis=-1, keepdims=True))
    inverse_std = lax.rsqrt(lax.optimization_barrier(jnp.mean(center * center, axis=-1, keepdims=True)) + 1e-06)
    normed = (center * inverse_std * gain).astype(jnp.bfloat16)
    before = jnp.dot(normed, expand, preferred_element_type=jnp.float32)
    active = jax.nn.gelu(before).astype(jnp.bfloat16)
    return jnp.dot(active, project, preferred_element_type=jnp.float32)

def cell_backward(hidden, gain, expand, project, mask_value, cotangent):
    center = hidden - lax.optimization_barrier(jnp.mean(hidden, axis=-1, keepdims=True))
    inverse_std = lax.rsqrt(lax.optimization_barrier(jnp.mean(center * center, axis=-1, keepdims=True)) + 1e-06)
    unit = center * inverse_std
    normed = (unit * gain).astype(jnp.bfloat16)
    before = jnp.dot(normed, expand, preferred_element_type=jnp.float32)
    masked = (mask_value[:, :, None] * cotangent).astype(jnp.bfloat16)
    active_adjoint = jnp.dot(masked, project.T, preferred_element_type=jnp.float32)
    _, gelu_back = jax.vjp(jax.nn.gelu, before)
    before_adjoint = gelu_back(active_adjoint)[0].astype(jnp.bfloat16)
    normed_adjoint = jnp.dot(before_adjoint, expand.T, preferred_element_type=jnp.float32)
    scaled = normed_adjoint * gain
    result = inverse_std * (scaled - lax.optimization_barrier(jnp.mean(scaled, axis=-1, keepdims=True)) - unit * lax.optimization_barrier(jnp.mean(scaled * unit, axis=-1, keepdims=True)))
    return result.astype(jnp.bfloat16)

def ocean_matrix(bands_row, blocks, lat_count):
    lat_band = blocks.shape[2]
    index = bands_row[:, None] * lat_band + jnp.arange(lat_band, dtype=jnp.int32)[None, :]
    onehot = (index[:, :, None] == jnp.arange(lat_count, dtype=jnp.int32)[None, None, :]).astype(jnp.float32)
    return jnp.einsum('poi,pia->oa', blocks, onehot, precision=lax.Precision.HIGHEST)

def atmosphere_matrix(bands_row, blocks, lat_count):
    lat_band = blocks.shape[1]
    index = bands_row[:, None] * lat_band + jnp.arange(lat_band, dtype=jnp.int32)[None, :]
    onehot = (index[:, :, None] == jnp.arange(lat_count, dtype=jnp.int32)[None, None, :]).astype(jnp.float32)
    return jnp.einsum('pio,pia->ao', blocks, onehot, precision=lax.Precision.HIGHEST)

def mix_complex(coefficient, mix_real, mix_imag):
    real_part = coefficient[:, :, 0].astype(jnp.float32)
    imag_part = coefficient[:, :, 1].astype(jnp.float32)
    first = mix_real.astype(jnp.float32)
    second = mix_imag.astype(jnp.float32)
    out_real = jnp.einsum('lmc,cd->lmd', real_part, first) - jnp.einsum('lmc,cd->lmd', imag_part, second)
    out_imag = jnp.einsum('lmc,cd->lmd', imag_part, first) + jnp.einsum('lmc,cd->lmd', real_part, second)
    return jnp.stack([out_real, out_imag], axis=2).astype(jnp.bfloat16)

def spectral_block(spectrum, forward, inverse, mixing):
    lat_count, columns, channels = spectrum.shape
    split = spectrum.reshape(lat_count, columns // 2, 2, channels).astype(jnp.float32)
    coefficient = jnp.einsum('mla,amrc->lmrc', forward.astype(jnp.float32), split).astype(jnp.bfloat16)
    mixed = mix_complex(coefficient, mixing[0], mixing[1])
    returned = jnp.einsum('mal,lmrc->amrc', inverse.astype(jnp.float32), mixed.astype(jnp.float32)).astype(jnp.bfloat16)
    return returned.reshape(lat_count, columns, channels)

def spectral_adjoint(returned_adjoint, forward, inverse, mixing):
    lat_count, columns, channels = returned_adjoint.shape
    split = returned_adjoint.reshape(lat_count, columns // 2, 2, channels).astype(jnp.float32)
    mixed_adjoint = jnp.einsum('mal,amrc->lmrc', inverse.astype(jnp.float32), split).astype(jnp.bfloat16)
    real_part = mixed_adjoint[:, :, 0].astype(jnp.float32)
    imag_part = mixed_adjoint[:, :, 1].astype(jnp.float32)
    first = mixing[0].astype(jnp.float32)
    second = mixing[1].astype(jnp.float32)
    back_real = jnp.einsum('lmd,cd->lmc', real_part, first) + jnp.einsum('lmd,cd->lmc', imag_part, second)
    back_imag = jnp.einsum('lmd,cd->lmc', imag_part, first) - jnp.einsum('lmd,cd->lmc', real_part, second)
    coefficient_adjoint = jnp.stack([back_real, back_imag], axis=2).astype(jnp.bfloat16)
    spectrum_adjoint = jnp.einsum('mla,lmrc->amrc', forward.astype(jnp.float32), coefficient_adjoint.astype(jnp.float32)).astype(jnp.bfloat16)
    return spectrum_adjoint.reshape(lat_count, columns, channels)

def ocean_layer(state, mask_value, kernel, gain, expand, project, band):
    radius = kernel.shape[0] // 2
    padded = jnp.pad(state, ((radius, radius), (0, 0), (0, 0)))
    band_count = state.shape[0] // band

    def one_band(index):
        start = index * band
        window = lax.dynamic_slice_in_dim(padded, start, band + 2 * radius, 0)
        update = cell_forward(depthwise(window, kernel), gain, expand, project)
        own = lax.dynamic_slice_in_dim(state, start, band, 0).astype(jnp.float32)
        weight = lax.dynamic_slice_in_dim(mask_value, start, band, 0)
        return (own + weight[:, :, None] * update).astype(jnp.bfloat16)
    result = lax.map(one_band, jnp.arange(band_count, dtype=jnp.int32))
    return result.reshape(state.shape)

def ocean_layer_adjoint(state, mask_value, kernel, gain, expand, project, cotangent, band):
    radius = kernel.shape[0] // 2
    padded = jnp.pad(state, ((radius, radius), (0, 0), (0, 0)))
    band_count = state.shape[0] // band

    def local_adjoint(index):
        start = index * band
        window = lax.dynamic_slice_in_dim(padded, start, band + 2 * radius, 0)
        hidden = depthwise(window, kernel)
        local_cotangent = lax.dynamic_slice_in_dim(cotangent, start, band, 0)
        weight = lax.dynamic_slice_in_dim(mask_value, start, band, 0)
        return cell_backward(hidden, gain, expand, project, weight, local_cotangent)
    hidden_adjoint = lax.map(local_adjoint, jnp.arange(band_count, dtype=jnp.int32)).reshape(state.shape)
    padded_adjoint = jnp.pad(hidden_adjoint, ((radius, radius), (0, 0), (0, 0)))
    flipped = kernel[::-1, ::-1]

    def spread(index):
        start = index * band
        window = lax.dynamic_slice_in_dim(padded_adjoint, start, band + 2 * radius, 0)
        return depthwise(window, flipped)
    spreads = lax.map(spread, jnp.arange(band_count, dtype=jnp.int32)).reshape(state.shape)
    return cotangent + spreads

def reference(atmosphere, ocean_state, land_mask, crossing_bands, ocean_regrid, atmosphere_regrid, surface_read, surface_embed, flux_read, flux_embed, legendre_forward, legendre_inverse, spectral_mix, conv_kernel, norm_gain, expand_weight, project_weight, atmosphere_cotangent, ocean_cotangent):
    group_total = crossing_bands.shape[0]
    lat_count, lon_count, channels = atmosphere.shape
    ocean_rows, ocean_lon, ocean_channels = ocean_state.shape
    band = ocean_rows // group_total
    ratio = ocean_lon // lon_count
    flux_count = flux_read.shape[1]
    highest = lax.Precision.HIGHEST
    to_ocean = jax.vmap(lambda row, blocks: ocean_matrix(row, blocks, lat_count))(crossing_bands, ocean_regrid)
    to_ocean = to_ocean.reshape(ocean_rows, lat_count)
    to_atmosphere = jax.vmap(lambda row, blocks: atmosphere_matrix(row, blocks, lat_count))(crossing_bands, atmosphere_regrid)
    to_atmosphere = jnp.transpose(to_atmosphere, (1, 0, 2)).reshape(lat_count, ocean_rows)
    mask_value = land_mask.astype(jnp.float32)
    surface = jnp.dot(ocean_state, surface_read, preferred_element_type=jnp.float32)
    coarse = lax.optimization_barrier(jnp.mean((mask_value * surface).reshape(ocean_rows, lon_count, ratio), axis=2))
    surface_atmosphere = jnp.dot(to_atmosphere, coarse, precision=highest)
    mixed_input = (atmosphere.astype(jnp.float32) + surface_atmosphere[:, :, None] * surface_embed[None, None, :]).astype(jnp.bfloat16)
    table = wave_table(lon_count, legendre_forward.shape[0]).astype(jnp.float32)
    spectrum = jnp.einsum('gk,agc->akc', table, mixed_input.astype(jnp.float32)).astype(jnp.bfloat16)
    returned = spectral_block(spectrum, legendre_forward, legendre_inverse, spectral_mix)
    response = jnp.einsum('gk,akc->agc', table, returned.astype(jnp.float32))
    atmosphere_next = (mixed_input.astype(jnp.float32) + jax.nn.gelu(response)).astype(jnp.bfloat16)
    flux = jnp.einsum('agc,cf->agf', atmosphere.astype(jnp.float32), flux_read.astype(jnp.float32))
    flux_ocean = jnp.dot(to_ocean, flux.reshape(lat_count, lon_count * flux_count), precision=highest)
    forcing_coarse = jnp.einsum('ogf,fc->ogc', flux_ocean.reshape(ocean_rows, lon_count, flux_count), flux_embed.astype(jnp.float32), precision=highest)
    forcing = jnp.broadcast_to(forcing_coarse[:, :, None, :], (ocean_rows, lon_count, ratio, ocean_channels)).reshape(ocean_rows, ocean_lon, ocean_channels)
    state = (ocean_state.astype(jnp.float32) + mask_value[:, :, None] * forcing).astype(jnp.bfloat16)
    states = []
    for layer in range(conv_kernel.shape[0]):
        states.append(state)
        state = ocean_layer(state, mask_value, conv_kernel[layer], norm_gain[layer], expand_weight[layer], project_weight[layer], band)
    ocean_next = state
    cotangent = ocean_cotangent.astype(jnp.float32)
    for layer in range(conv_kernel.shape[0] - 1, -1, -1):
        cotangent = ocean_layer_adjoint(states[layer], mask_value, conv_kernel[layer], norm_gain[layer], expand_weight[layer], project_weight[layer], cotangent, band)
    forcing_adjoint = (mask_value[:, :, None] * cotangent).reshape(ocean_rows, lon_count, ratio, ocean_channels).sum(axis=2)
    flux_ocean_adjoint = jnp.einsum('ogc,fc->ogf', forcing_adjoint, flux_embed.astype(jnp.float32), precision=highest)
    flux_adjoint = jnp.dot(to_ocean.T, flux_ocean_adjoint.reshape(ocean_rows, lon_count * flux_count), precision=highest)
    flux_adjoint = flux_adjoint.reshape(lat_count, lon_count, flux_count)
    from_flux = jnp.einsum('agf,cf->agc', flux_adjoint, flux_read.astype(jnp.float32), precision=highest)
    atmosphere_adjoint = atmosphere_cotangent.astype(jnp.float32)
    _, gelu_back = jax.vjp(jax.nn.gelu, response)
    response_adjoint = gelu_back(atmosphere_adjoint)[0].astype(jnp.bfloat16)
    returned_adjoint = jnp.einsum('gk,agc->akc', table, response_adjoint.astype(jnp.float32)).astype(jnp.bfloat16)
    spectrum_adjoint = spectral_adjoint(returned_adjoint, legendre_forward, legendre_inverse, spectral_mix)
    input_adjoint = atmosphere_adjoint + jnp.einsum('gk,akc->agc', table, spectrum_adjoint.astype(jnp.float32))
    atmosphere_grad = input_adjoint + from_flux
    surface_adjoint = jnp.einsum('agc,c->ag', input_adjoint, surface_embed, precision=highest)
    coarse_adjoint = jnp.dot(to_atmosphere.T, surface_adjoint, precision=highest)
    widened = jnp.broadcast_to(coarse_adjoint[:, :, None], (ocean_rows, lon_count, ratio)).reshape(ocean_rows, ocean_lon)
    surface_grad = mask_value * widened / ratio
    ocean_grad = cotangent + surface_grad[:, :, None] * surface_read.astype(jnp.float32)[None, None, :]
    return (atmosphere_next, ocean_next, atmosphere_grad, ocean_grad)
```

```python
import jax
import jax.numpy as jnp
from jax import lax
from jax.experimental import pallas as pl
from jax.experimental.pallas import tpu as pltpu
from jax.sharding import PartitionSpec as P


def with_halo(x, sides, width, wrap):
    for axis, dim in sides:
        size, length = (lax.axis_size(axis), x.shape[dim])
        up = [(i, (i + 1) % size) for i in range(size if wrap else size - 1)]
        down = [(j, i) for i, j in up]
        last = lax.slice_in_dim(x, length - width, length, axis=dim)
        first = lax.slice_in_dim(x, 0, width, axis=dim)
        before = lax.ppermute(last, axis, up)
        after = lax.ppermute(first, axis, down)
        x = jnp.concatenate([before, x, after], axis=dim)
    return x


def wave_table(lon_count, mode_count):
    longitude = jnp.arange(lon_count, dtype=jnp.int32)
    wavenumber = jnp.arange(mode_count, dtype=jnp.int32)
    phase = (longitude[:, None] * wavenumber[None, :] % lon_count).astype(jnp.float32) * (
        2.0 * jnp.pi / lon_count
    )
    scaled = jnp.stack([jnp.cos(phase), -jnp.sin(phase)], axis=2) * jnp.sqrt(
        jnp.float32(2.0 / lon_count)
    )
    return scaled.reshape(lon_count, 2 * mode_count).astype(jnp.bfloat16)


GELU_SCALE = 0.7978845608028654
GELU_CUBIC = 0.044715


def conv_into(window, taps, store, side):
    rows = window.shape[0] - side + 1
    extent = window.shape[1] - side + 1

    def step(index, carry):
        start = pl.multiple_of(index * 8, 8)
        totals = [None] * rows
        for col in range(side):
            weights = [taps[row * side + col] for row in range(side)]
            for line in range(rows + side - 1):
                piece = window[line, pl.ds(start + col, 8), :]
                for row in range(side):
                    target = line - row
                    if 0 <= target < rows:
                        term = piece * weights[row]
                        totals[target] = term if totals[target] is None else totals[target] + term
        for row in range(rows):
            store(row, start, totals[row])
        return carry

    lax.fori_loop(0, extent // 8, step, jnp.int32(0))


def widen(narrow, wide):
    def step(line, carry):
        wide[line] = narrow[line].astype(jnp.float32)
        return carry

    lax.fori_loop(0, narrow.shape[0], step, jnp.int32(0))


def forward_kernel(
    narrow, taps, mask, gain, expand, project, state_out, hidden_out, window
):
    widen(narrow, window)
    rows, extent, _ = state_out.shape
    side = window.shape[0] - rows + 1
    radius = side // 2

    def store(row, start, value):
        hidden_out[row, pl.ds(start, 8), :] = value

    conv_into(window, taps, store, side)

    def cells(row, carry):
        hidden = hidden_out[row]
        center = hidden - jnp.mean(hidden, axis=-1, keepdims=True)
        inverse_std = lax.rsqrt(jnp.mean(center * center, axis=-1, keepdims=True) + 1e-06)
        normed = (center * inverse_std * gain[...]).astype(jnp.bfloat16)
        before = jnp.dot(normed, expand[...], preferred_element_type=jnp.float32)
        inner = before * (GELU_SCALE + (GELU_SCALE * GELU_CUBIC) * (before * before))
        scaled = 0.5 * before
        active = (scaled + scaled * jnp.tanh(inner)).astype(jnp.bfloat16)
        update = jnp.dot(active, project[...], preferred_element_type=jnp.float32)
        old = window[row + radius, radius : radius + extent, :]
        state_out[row] = (old + mask[row].astype(jnp.float32) * update).astype(jnp.bfloat16)
        return carry

    lax.fori_loop(0, rows, cells, jnp.int32(0))


def cell_backward(hidden, cotangent, mask, gain, expand, expand_t, project_t):
    center = hidden - jnp.mean(hidden, axis=-1, keepdims=True)
    inverse_std = lax.rsqrt(jnp.mean(center * center, axis=-1, keepdims=True) + 1e-06)
    unit = center * inverse_std
    normed = (unit * gain).astype(jnp.bfloat16)
    before = jnp.dot(normed, expand, preferred_element_type=jnp.float32)
    masked = (mask.astype(jnp.float32) * cotangent).astype(jnp.bfloat16)
    active_adjoint = jnp.dot(masked, project_t, preferred_element_type=jnp.float32)
    square = before * before
    wave = jnp.tanh(before * (GELU_SCALE + (GELU_SCALE * GELU_CUBIC) * square))
    slope = (0.5 * GELU_SCALE + (1.5 * GELU_SCALE * GELU_CUBIC) * square) * before
    derivative = 0.5 + 0.5 * wave + slope * (1.0 - wave * wave)
    before_adjoint = (derivative * active_adjoint).astype(jnp.bfloat16)
    scaled = jnp.dot(before_adjoint, expand_t, preferred_element_type=jnp.float32) * gain
    return (
        inverse_std
        * (
            scaled
            - jnp.mean(scaled, axis=-1, keepdims=True)
            - unit * jnp.mean(scaled * unit, axis=-1, keepdims=True)
        )
    ).astype(jnp.bfloat16)


def backward_kernel(hidden, cotangent, mask, gain, expand, expand_t, project_t, adjoint_out):
    def cells(row, carry):
        adjoint_out[row] = cell_backward(
            hidden[row],
            cotangent[row].astype(jnp.float32),
            mask[row],
            gain[...],
            expand[...],
            expand_t[...],
            project_t[...],
        )
        return carry

    lax.fori_loop(0, hidden.shape[0], cells, jnp.int32(0))


def adjoint_kernel(narrow, taps, cotangent, cotangent_out, window):
    widen(narrow, window)
    side = window.shape[0] - cotangent.shape[0] + 1

    def store(row, start, value):
        old = cotangent[row, pl.ds(start, 8), :].astype(jnp.float32)
        cotangent_out[row, pl.ds(start, 8), :] = old + value

    conv_into(window, taps, store, side)


def adjoint_backward_kernel(
    narrow, taps, cotangent, hidden, mask, gain, expand, expand_t, project_t,
    cotangent_out, adjoint_out, window,
):
    adjoint_kernel(narrow, taps, cotangent, cotangent_out, window)
    backward_kernel(
        hidden, cotangent_out, mask, gain, expand, expand_t, project_t, adjoint_out
    )


def run_kernel(kernel, outs, flops, *operands, scratch=()):
    size = sum(x.size * x.dtype.itemsize for x in operands)
    return pl.pallas_call(
        kernel,
        out_shape=outs,
        in_specs=[pl.BlockSpec(memory_space=pltpu.VMEM)] * len(operands),
        scratch_shapes=list(scratch),
        out_specs=jax.tree.map(lambda _: pl.BlockSpec(memory_space=pltpu.VMEM), outs),
        cost_estimate=pl.CostEstimate(flops=flops, bytes_accessed=size, transcendentals=0),
    )(*operands)


def tap_tiles(kernel):
    side, _, channels = kernel.shape
    flat = kernel.astype(jnp.float32).reshape(side * side, 1, channels)
    return jnp.broadcast_to(flat, (side * side, 8, channels))


def ocean_matrix(bands_row, blocks, lat_count):
    lat_band = blocks.shape[2]
    index = bands_row[:, None] * lat_band + jnp.arange(lat_band, dtype=jnp.int32)[None, :]
    onehot = (index[:, :, None] == jnp.arange(lat_count, dtype=jnp.int32)[None, None, :]).astype(
        jnp.float32
    )
    return jnp.einsum("poi,pia->oa", blocks, onehot, precision=lax.Precision.HIGHEST)


def atmosphere_matrix(bands_row, blocks, lat_count):
    lat_band = blocks.shape[1]
    index = bands_row[:, None] * lat_band + jnp.arange(lat_band, dtype=jnp.int32)[None, :]
    onehot = (index[:, :, None] == jnp.arange(lat_count, dtype=jnp.int32)[None, None, :]).astype(
        jnp.float32
    )
    return jnp.einsum("pio,pia->ao", blocks, onehot, precision=lax.Precision.HIGHEST)


def mix_complex(coefficient, mix_real, mix_imag):
    real_part = coefficient[:, :, 0]
    imag_part = coefficient[:, :, 1]
    out_real = jnp.einsum(
        "lmc,cd->lmd", real_part, mix_real, preferred_element_type=jnp.float32
    ) - jnp.einsum("lmc,cd->lmd", imag_part, mix_imag, preferred_element_type=jnp.float32)
    out_imag = jnp.einsum(
        "lmc,cd->lmd", imag_part, mix_real, preferred_element_type=jnp.float32
    ) + jnp.einsum("lmc,cd->lmd", real_part, mix_imag, preferred_element_type=jnp.float32)
    return jnp.stack([out_real, out_imag], axis=2).astype(jnp.bfloat16)


def spectral_block(spectrum, forward, inverse, mixing):
    lat_count, columns, channels = spectrum.shape
    split = spectrum.reshape(lat_count, columns // 2, 2, channels)
    coefficient = jnp.einsum(
        "mla,amrc->lmrc", forward, split, preferred_element_type=jnp.float32
    ).astype(jnp.bfloat16)
    mixed = mix_complex(coefficient, mixing[0], mixing[1])
    returned = jnp.einsum(
        "mal,lmrc->amrc", inverse, mixed, preferred_element_type=jnp.float32
    ).astype(jnp.bfloat16)
    return returned.reshape(lat_count, columns, channels)


def spectral_adjoint(returned_adjoint, forward, inverse, mixing):
    lat_count, columns, channels = returned_adjoint.shape
    split = returned_adjoint.reshape(lat_count, columns // 2, 2, channels)
    mixed_adjoint = jnp.einsum(
        "mal,amrc->lmrc", inverse, split, preferred_element_type=jnp.float32
    ).astype(jnp.bfloat16)
    real_part = mixed_adjoint[:, :, 0]
    imag_part = mixed_adjoint[:, :, 1]
    back_real = jnp.einsum(
        "lmd,cd->lmc", real_part, mixing[0], preferred_element_type=jnp.float32
    ) + jnp.einsum("lmd,cd->lmc", imag_part, mixing[1], preferred_element_type=jnp.float32)
    back_imag = jnp.einsum(
        "lmd,cd->lmc", imag_part, mixing[0], preferred_element_type=jnp.float32
    ) - jnp.einsum("lmd,cd->lmc", real_part, mixing[1], preferred_element_type=jnp.float32)
    coefficient_adjoint = jnp.stack([back_real, back_imag], axis=2).astype(jnp.bfloat16)
    spectrum_adjoint = jnp.einsum(
        "mla,lmrc->amrc", forward, coefficient_adjoint, preferred_element_type=jnp.float32
    ).astype(jnp.bfloat16)
    return spectrum_adjoint.reshape(lat_count, columns, channels)


def to_modes(values):
    return lax.all_to_all(values, ("sec", "tile"), split_axis=1, concat_axis=0, tiled=True)


def to_bands(values):
    return lax.all_to_all(values, ("sec", "tile"), split_axis=0, concat_axis=1, tiled=True)


def rims(values, width):
    with_rows = with_halo(values, (("tile", 0),), width, False)
    return with_halo(with_rows, (("sec", 1),), width, True)


def swap(values):
    return lax.all_to_all(values, ("sec", "tile"), split_axis=0, concat_axis=0, tiled=True)


def for_halves(values, sections):
    lat_rows = values.shape[0]
    parts = jnp.moveaxis(values.reshape(lat_rows, sections, -1), 1, 0)
    tiles = lax.axis_size("tile")
    spread = jnp.broadcast_to(parts[:, None], (sections, tiles) + parts.shape[1:])
    return spread.reshape((sections * tiles,) + parts.shape[1:])


def sum_halves(received, sections):
    count, lat_rows, width = received.shape
    total = received.reshape(sections, count // sections, lat_rows, width).sum(axis=1)
    return jnp.moveaxis(total, 0, 1).reshape(lat_rows, sections * width)


def per_device(
    atmosphere,
    ocean_state,
    land_mask,
    crossing_bands,
    ocean_regrid,
    atmosphere_regrid,
    surface_read,
    surface_embed,
    flux_read,
    flux_embed,
    legendre_forward,
    legendre_inverse,
    spectral_mix,
    conv_kernel,
    norm_gain,
    expand_weight,
    project_weight,
    atmosphere_cotangent,
    ocean_cotangent,
):
    band_total = lax.axis_size(("sec", "tile"))
    lat_rows, lon_count, channels = atmosphere.shape
    lat_count = lat_rows * band_total
    ocean_rows, ocean_lon, ocean_channels = ocean_state.shape
    half = lon_count // lax.axis_size("sec")
    ratio = ocean_lon // half
    flux_count = flux_read.shape[1]
    radius = conv_kernel.shape[1] // 2
    layer_count = conv_kernel.shape[0]
    highest = lax.Precision.HIGHEST
    mask_value = land_mask.astype(jnp.float32)
    to_ocean = ocean_matrix(crossing_bands[0], ocean_regrid[0], lat_count)
    to_atmosphere = atmosphere_matrix(crossing_bands[0], atmosphere_regrid[0], lat_count)
    surface = jnp.dot(ocean_state, surface_read, preferred_element_type=jnp.float32)
    coarse = jnp.mean((mask_value * surface).reshape(ocean_rows, half, ratio), axis=2)
    sections = lax.axis_size("sec")
    flux = jnp.einsum("agc,cf->agf", atmosphere, flux_read, preferred_element_type=jnp.float32)
    coarse_parts = jnp.dot(to_atmosphere, coarse, precision=highest)
    arrived = swap(
        jnp.concatenate(
            [
                for_halves(flux.reshape(lat_rows, lon_count * flux_count), sections),
                coarse_parts.reshape(band_total, lat_rows, half),
            ],
            axis=2,
        )
    )
    flux_width = half * flux_count
    surface_atmosphere = sum_halves(arrived[:, :, flux_width:], sections)
    flux_ocean = jnp.dot(
        to_ocean, arrived[:, :, :flux_width].reshape(lat_count, flux_width), precision=highest
    )
    mixed_input = (
        atmosphere.astype(jnp.float32)
        + surface_atmosphere[:, :, None] * surface_embed[None, None, :]
    ).astype(jnp.bfloat16)
    table = wave_table(lon_count, legendre_forward.shape[0] * band_total)
    spectrum = jnp.einsum(
        "gk,agc->akc", table, mixed_input, preferred_element_type=jnp.float32
    ).astype(jnp.bfloat16)
    returned = to_bands(
        spectral_block(to_modes(spectrum), legendre_forward, legendre_inverse, spectral_mix)
    )
    response = jnp.einsum("gk,akc->agc", table, returned, preferred_element_type=jnp.float32)
    atmosphere_next = (mixed_input.astype(jnp.float32) + jax.nn.gelu(response)).astype(jnp.bfloat16)
    forcing_coarse = jnp.einsum(
        "ogf,fc->ogc",
        flux_ocean.reshape(ocean_rows, half, flux_count),
        flux_embed.astype(jnp.float32),
        precision=highest,
    )
    forcing = jnp.broadcast_to(
        forcing_coarse[:, :, None, :], (ocean_rows, half, ratio, ocean_channels)
    ).reshape(ocean_rows, ocean_lon, ocean_channels)
    state = (ocean_state.astype(jnp.float32) + mask_value[:, :, None] * forcing).astype(
        jnp.bfloat16
    )
    mask_wide = jnp.broadcast_to(
        mask_value[:, :, None], (ocean_rows, ocean_lon, ocean_channels)
    ).astype(jnp.bfloat16)
    shape = (ocean_rows, ocean_lon, ocean_channels)
    narrow = jax.ShapeDtypeStruct(shape, jnp.bfloat16)
    wide = jax.ShapeDtypeStruct(shape, jnp.float32)
    hidden_units = expand_weight.shape[2]
    work = ocean_rows * ocean_lon * ocean_channels
    conv_flops = 2000 * work
    cell_flops = 8 * work * hidden_units
    gains = norm_gain[:, None, :]
    hiddens = []
    window_scratch = (
        pltpu.VMEM(
            (ocean_rows + 2 * radius, ocean_lon + 2 * radius, ocean_channels), jnp.float32
        ),
    )
    for layer in range(layer_count):
        state, hidden = run_kernel(
            forward_kernel,
            (narrow, wide),
            conv_flops + cell_flops,
            rims(state, radius),
            tap_tiles(conv_kernel[layer]),
            mask_wide,
            gains[layer],
            expand_weight[layer],
            project_weight[layer],
            scratch=window_scratch,
        )
        hiddens.append(hidden)

    def cell_operands(layer):
        return (
            mask_wide,
            gains[layer],
            expand_weight[layer],
            expand_weight[layer].T,
            project_weight[layer].T,
        )

    def conv_operands(layer, adjoint):
        return (
            rims(adjoint, radius),
            tap_tiles(conv_kernel[layer, ::-1, ::-1]),
        )

    last = layer_count - 1
    cotangent = ocean_cotangent
    hidden_adjoint = run_kernel(
        backward_kernel,
        narrow,
        2 * cell_flops,
        hiddens[last],
        cotangent,
        *cell_operands(last),
    )
    for layer in range(last, 0, -1):
        cotangent, hidden_adjoint = run_kernel(
            adjoint_backward_kernel,
            (wide, narrow),
            conv_flops + 2 * cell_flops,
            *conv_operands(layer, hidden_adjoint),
            cotangent,
            hiddens[layer - 1],
            *cell_operands(layer - 1),
            scratch=window_scratch,
        )
    cotangent = run_kernel(
        adjoint_kernel,
        wide,
        conv_flops,
        *conv_operands(0, hidden_adjoint),
        cotangent,
        scratch=window_scratch,
    )
    forcing_adjoint = (
        (mask_value[:, :, None] * cotangent)
        .reshape(ocean_rows, half, ratio, ocean_channels)
        .sum(axis=2)
    )
    flux_ocean_adjoint = jnp.einsum(
        "ogc,fc->ogf", forcing_adjoint, flux_embed.astype(jnp.float32), precision=highest
    )
    flux_parts = jnp.dot(
        to_ocean.T, flux_ocean_adjoint.reshape(ocean_rows, flux_width), precision=highest
    )
    flux_adjoint = sum_halves(
        swap(flux_parts.reshape(band_total, lat_rows, flux_width)), sections
    ).reshape(lat_rows, lon_count, flux_count)
    from_flux = jnp.einsum(
        "agf,cf->agc", flux_adjoint, flux_read.astype(jnp.float32), precision=highest
    )
    atmosphere_adjoint = atmosphere_cotangent.astype(jnp.float32)
    _, gelu_back = jax.vjp(jax.nn.gelu, response)
    response_adjoint = gelu_back(atmosphere_adjoint)[0].astype(jnp.bfloat16)
    returned_adjoint = jnp.einsum(
        "gk,agc->akc", table, response_adjoint, preferred_element_type=jnp.float32
    ).astype(jnp.bfloat16)
    spectrum_adjoint = to_bands(
        spectral_adjoint(
            to_modes(returned_adjoint), legendre_forward, legendre_inverse, spectral_mix
        )
    )
    input_adjoint = atmosphere_adjoint + jnp.einsum(
        "gk,akc->agc", table, spectrum_adjoint, preferred_element_type=jnp.float32
    )
    atmosphere_grad = input_adjoint + from_flux
    surface_adjoint = jnp.einsum("agc,c->ag", input_adjoint, surface_embed, precision=highest)
    coarse_adjoint = jnp.dot(
        to_atmosphere.T,
        swap(for_halves(surface_adjoint, sections)).reshape(lat_count, half),
        precision=highest,
    )
    widened_adjoint = jnp.broadcast_to(
        coarse_adjoint[:, :, None], (ocean_rows, half, ratio)
    ).reshape(ocean_rows, ocean_lon)
    surface_grad = mask_value * widened_adjoint / ratio
    ocean_grad = (
        cotangent + surface_grad[:, :, None] * surface_read.astype(jnp.float32)[None, None, :]
    )
    return (atmosphere_next, state, atmosphere_grad, ocean_grad)


def solution(mesh):
    return jax.shard_map(
        per_device,
        mesh=mesh,
        in_specs=(
            P(("sec", "tile"), None, None),
            P("tile", "sec", None),
            P("tile", "sec"),
            P("tile", None),
            P("tile", None, None, None),
            P("tile", None, None, None),
            P(),
            P(),
            P(),
            P(),
            P(("sec", "tile"), None, None),
            P(("sec", "tile"), None, None),
            P(),
            P(),
            P(),
            P(),
            P(),
            P(("sec", "tile"), None, None),
            P("tile", "sec", None),
        ),
        out_specs=(
            P(("sec", "tile"), None, None),
            P("tile", "sec", None),
            P(("sec", "tile"), None, None),
            P("tile", "sec", None),
        ),
        check_vma=False,
    )
```
